32 devices in a mesh: unit: 4 (over y, x), replica: 2 (over core), model: 4 (over z).
Axes of the slice: x: 2, y: 2, z: 4, core: 2. Of those that a mesh axis runs over, the one named last changes fastest.
Arguments:
- slope_up: float32 [8, 768, 3072], P(('unit', 'replica'), None, 'model'), parts along dimension 0, may hold values from -0.875 to 0.875
- slope_down: float32 [8, 3072, 768], P(('unit', 'replica'), 'model'), parts along dimension 0, may hold values from -0.875 to 0.875
- slope_query: float32 [8, 768, 768], P(('unit', 'replica'), None, 'model'), parts along dimension 0, may hold values from -0.875 to 0.875
- slope_key: float32 [8, 768, 768], P(('unit', 'replica'), None, 'model'), parts along dimension 0, may hold values from -0.875 to 0.875
- slope_value: float32 [8, 768, 768], P(('unit', 'replica'), None, 'model'), parts along dimension 0, may hold values from -0.875 to 0.875
- slope_mixed: float32 [8, 768, 768], P(('unit', 'replica'), 'model'), parts along dimension 0, may hold values from -0.875 to 0.875
- slope_norm: float32 [8, 768], P(('unit', 'replica')), parts along dimension 0, may hold values from -8 to 8
- param_up: float32 [3072, 3072], P(('unit', 'replica'), 'model'), parts along dimension 0, may hold values from -0.21875 to 0.21875
- param_down: float32 [12288, 768], P(('unit', 'model'), 'replica'), parts along dimension 0, may hold values from -0.109375 to 0.109375
- param_query: float32 [3072, 768], P(('unit', 'replica'), 'model'), parts along dimension 0, may hold values from -0.21875 to 0.21875
- param_key: float32 [3072, 768], P(('unit', 'replica'), 'model'), parts along dimension 0, may hold values from -0.21875 to 0.21875
- param_value: float32 [3072, 768], P(('unit', 'replica'), 'model'), parts along dimension 0, may hold values from -0.21875 to 0.21875
- param_mixed: float32 [3072, 768], P(('unit', 'model'), 'replica'), parts along dimension 0, may hold values from -0.21875 to 0.21875
- param_norm: float32 [3072], P(('unit', 'replica')), parts along dimension 0, may hold values from 0.25 to 1.75
Outputs:
- half_up: bfloat16 [3072, 3072], P('unit', 'model'), parts along dimension 0
- half_down: bfloat16 [12288, 768], P(('unit', 'model')), parts along dimension 0
- half_query: bfloat16 [3072, 768], P('unit', 'model'), parts along dimension 0
- half_key: bfloat16 [3072, 768], P('unit', 'model'), parts along dimension 0
- half_value: bfloat16 [3072, 768], P('unit', 'model'), parts along dimension 0
- half_mixed: bfloat16 [3072, 768], P(('unit', 'model')), parts along dimension 0
- half_norm: bfloat16 [3072], P('unit'), parts along dimension 0
- next_up: float32 [3072, 3072], P(('unit', 'replica'), 'model'), parts along dimension 0
- next_down: float32 [12288, 768], P(('unit', 'model'), 'replica'), parts along dimension 0
- next_query: float32 [3072, 768], P(('unit', 'replica'), 'model'), parts along dimension 0
- next_key: float32 [3072, 768], P(('unit', 'replica'), 'model'), parts along dimension 0
- next_value: float32 [3072, 768], P(('unit', 'replica'), 'model'), parts along dimension 0
- next_mixed: float32 [3072, 768], P(('unit', 'model'), 'replica'), parts along dimension 0
- next_norm: float32 [3072], P(('unit', 'replica')), parts along dimension 0
The draws below stay inside these ranges and needn't reach their ends.
There are 4 independent parts, one for each index of `unit`. The reference program is written for one: setup_inputs(seed, part) draws one part's arguments, and reference() takes and returns one part's arrays. A program takes and returns all parts, laid end to end along the dimension named above; each array names one. Nothing has to cross between parts.
All inputs are finite; a program needn't handle non-finite values.
Results may differ from the reference program's by a relative error of at most 0.001.
Values may be sent and summed in bfloat16 or wider, within the bound.
A program may use at most 64 MiB of HBM per device.

```python
import jax
import jax.numpy as jnp

WIDTH = 768
INNER = 3072
ATTN = 768
REPLICAS = 2


def spiked(array, stream_key, source, target, shards_of, factor):
    owner, partner = [(jnp.arange(array.shape[axis_at]) // (array.shape[axis_at] // shards_of)).reshape([-1 if axis == axis_at else 1 for axis in range(array.ndim)]) for axis_at in (source, target)]
    chosen = jax.random.permutation(stream_key, shards_of)[partner]
    strong = (owner == chosen) | (owner == (partner + shards_of // 2) % shards_of)
    return jnp.where(strong, factor * array, array)


def block_levels(key, shape, split, low, largest):
    gain, own = 1.0, jax.random.fold_in(key, 6)
    for axis_at, parts in split:
        heights = jnp.exp(jax.random.uniform(jax.random.fold_in(own, axis_at), (parts,), jnp.float32, low / len(split), largest / len(split)))
        gain = gain * jnp.repeat(heights, shape[axis_at] // parts).reshape([-1 if axis == axis_at else 1 for axis in range(len(shape))])
    return gain


def centred(stream_key, extent, deviation, reach, split=(), kind=jnp.bfloat16):
    entries = deviation * jax.random.normal(stream_key, extent, jnp.float32)
    if split:
        entries = entries * block_levels(stream_key, extent, split, -0.22, 0.18)
    return jnp.clip(entries, -reach, reach).astype(kind)


def noise_with(stream_key, dims, scale, most, pieces, heavy, dtype=jnp.bfloat16):
    values = scale * jax.random.normal(stream_key, dims, jnp.float32)
    if pieces:
        values = values * block_levels(stream_key, dims, pieces, -0.22, 0.18)
    return jnp.clip(spiked(values, jax.random.fold_in(stream_key, 3), *heavy), -most, most).astype(dtype)


def setup_inputs(seed: int = 0, part: int = 0) -> dict:
    streams_of = jax.random.split(jax.random.key(seed), 15)
    part_keys = jax.random.split(jax.random.fold_in(streams_of[14], part), 15)
    return {
        "slope_up": noise_with(part_keys[0], (REPLICAS, WIDTH, INNER), 0.1, 0.875, ((0, 2), (2, 4)), (0, 1, 2, 2.0), jnp.float32),
        "slope_down": noise_with(part_keys[1], (REPLICAS, INNER, WIDTH), 0.1, 0.875, ((0, 2), (1, 4)), (0, 2, 2, 2.0), jnp.float32),
        "slope_query": noise_with(part_keys[2], (REPLICAS, WIDTH, ATTN), 0.1, 0.875, ((0, 2), (2, 4)), (0, 1, 2, 2.0), jnp.float32),
        "slope_key": noise_with(part_keys[3], (REPLICAS, WIDTH, ATTN), 0.1, 0.875, ((0, 2), (2, 4)), (0, 1, 2, 2.0), jnp.float32),
        "slope_value": noise_with(part_keys[4], (REPLICAS, WIDTH, ATTN), 0.1, 0.875, ((0, 2), (2, 4)), (0, 1, 2, 2.0), jnp.float32),
        "slope_mixed": noise_with(part_keys[5], (REPLICAS, ATTN, WIDTH), 0.1, 0.875, ((0, 2), (1, 4)), (0, 2, 2, 2.0), jnp.float32),
        "slope_norm": noise_with(part_keys[6], (REPLICAS, WIDTH), 1.0, 8.0, ((0, 2),), (0, 1, 2, 2.0), jnp.float32),
        "param_up": centred(part_keys[7], (WIDTH, INNER), WIDTH ** -0.5, 0.21875, ((0, 2), (1, 4)), jnp.float32),
        "param_down": centred(part_keys[8], (INNER, WIDTH), INNER ** -0.5, 0.109375, ((0, 4), (1, 2)), jnp.float32),
        "param_query": centred(part_keys[9], (WIDTH, ATTN), WIDTH ** -0.5, 0.21875, ((0, 2), (1, 4)), jnp.float32),
        "param_key": centred(part_keys[10], (WIDTH, ATTN), WIDTH ** -0.5, 0.21875, ((0, 2), (1, 4)), jnp.float32),
        "param_value": centred(part_keys[11], (WIDTH, ATTN), WIDTH ** -0.5, 0.21875, ((0, 2), (1, 4)), jnp.float32),
        "param_mixed": centred(part_keys[12], (ATTN, WIDTH), ATTN ** -0.5, 0.21875, ((0, 4), (1, 2)), jnp.float32),
        "param_norm": jnp.clip(1.0 + 0.15 * jax.random.normal(part_keys[13], (WIDTH,), jnp.float32), 0.25, 1.75),
    }


learn_rate = 0.3


def reference(slope_up, slope_down, slope_query, slope_key, slope_value, slope_mixed, slope_norm, param_up, param_down, param_query, param_key, param_value, param_mixed, param_norm):
    mean_up = jnp.sum(slope_up.astype(jnp.float32), axis=0) * REPLICAS ** -0.5
    mean_down = jnp.sum(slope_down.astype(jnp.float32), axis=0) * REPLICAS ** -0.5
    mean_query = jnp.sum(slope_query.astype(jnp.float32), axis=0) * REPLICAS ** -0.5
    mean_key = jnp.sum(slope_key.astype(jnp.float32), axis=0) * REPLICAS ** -0.5
    mean_value = jnp.sum(slope_value.astype(jnp.float32), axis=0) * REPLICAS ** -0.5
    mean_mixed = jnp.sum(slope_mixed.astype(jnp.float32), axis=0) * REPLICAS ** -0.5
    mean_norm = jnp.sum(slope_norm.astype(jnp.float32), axis=0) * REPLICAS ** -0.5
    next_up = param_up - learn_rate * mean_up
    next_down = param_down - learn_rate * mean_down
    next_query = param_query - learn_rate * mean_query
    next_key = param_key - learn_rate * mean_key
    next_value = param_value - learn_rate * mean_value
    next_mixed = param_mixed - learn_rate * mean_mixed
    next_norm = param_norm - learn_rate * mean_norm
    half_up = next_up.astype(jnp.bfloat16)
    half_down = next_down.astype(jnp.bfloat16)
    half_query = next_query.astype(jnp.bfloat16)
    half_key = next_key.astype(jnp.bfloat16)
    half_value = next_value.astype(jnp.bfloat16)
    half_mixed = next_mixed.astype(jnp.bfloat16)
    half_norm = next_norm.astype(jnp.bfloat16)
    return half_up, half_down, half_query, half_key, half_value, half_mixed, half_norm, next_up, next_down, next_query, next_key, next_value, next_mixed, next_norm
```

```python
import functools

import jax
import jax.numpy as jnp
from jax import lax
from jax.experimental import pallas as pl
from jax.experimental.pallas import tpu as pltpu
from jax.sharding import PartitionSpec as P

learn_rate = 0.3
LOG2E = 1.4426950408889634
ANY = pl.BlockSpec(memory_space=pl.ANY)
VMEM_BYTES = 67043328


def plan(halves, size):
    chunks = []
    for at, (rows, columns) in enumerate(halves):
        parts = max(1, rows * columns // size)
        if rows % (16 * parts):
            parts = 1
        chunks += [(at, part * (rows // parts), rows // parts) for part in range(parts)]
    return chunks


def block(rows, columns, size):
    step = rows
    while step % 32 == 0 and step * columns > size:
        step //= 2
    return step


def coded(slope):
    scaled = slope * 256.0
    square = scaled * scaled
    fourth = square * square
    eighth = fourth * fourth
    size = jnp.maximum(eighth, eighth * eighth)
    return jnp.where(slope < 0.0, -size, size).astype(jnp.bfloat16)


def decoded(code):
    code = code.astype(jnp.float32)
    power = jnp.log(jnp.abs(code))
    size = jnp.exp2(jnp.minimum(power * (LOG2E / 8), power * (LOG2E / 16)) - 8.0)
    return jnp.where(code < 0.0, -size, size)


def exchange(n, by_row, chunks, size, rate, *refs):
    m = len(by_row)
    slopes, slope_norm = refs[:m], refs[m]
    params, param_norm = refs[m + 1 : 2 * m + 1], refs[2 * m + 1]
    refs = refs[2 * m + 2 :]
    halfs, norm_half = refs[:m], refs[m]
    kept, norm_next = refs[m + 1 : 2 * m + 1], refs[2 * m + 1]
    refs = refs[2 * m + 2 :]
    own, away, code, got = refs[:m], refs[m : 2 * m], refs[2 * m : 3 * m], refs[3 * m : 4 * m]
    (norms, norm_own, norm_got, norm_all, away_sem, own_sem, keep_sem, send_sem, recv_sem,
     back_send, back_recv, norm_in, norm_send, norm_recv) = refs[4 * m :]

    me = lax.axis_index("replica")
    peer = 1 - me
    there = {"replica": peer}

    def half_of(at, who, start, rows):
        height, width = kept[at].shape
        if by_row[at]:
            return pl.ds(pl.multiple_of(who * height + start, 16), rows), pl.ds(0, width)
        return pl.ds(start, rows), pl.ds(pl.multiple_of(who * width, width), width)

    def remote(source, target, out_sem, in_sem):
        return pltpu.make_async_remote_copy(
            src_ref=source,
            dst_ref=target,
            send_sem=out_sem,
            recv_sem=in_sem,
            device_id=there,
            device_id_type=pl.DeviceIdType.MESH,
        )

    fetches, loads, sends = [], [], []
    for c, (at, start, rows) in enumerate(chunks):
        mine = pl.ds(start, rows)
        fetches.append(pltpu.make_async_copy(
            slopes[at].at[(0, *half_of(at, peer, start, rows))], away[at].at[mine], away_sem.at[c]
        ))
        loads.append((
            pltpu.make_async_copy(
                slopes[at].at[(0, *half_of(at, me, start, rows))], own[at].at[mine], own_sem.at[c]
            ),
            pltpu.make_async_copy(params[at].at[mine], kept[at].at[mine], keep_sem.at[c]),
        ))
        sends.append(remote(code[at].at[mine], got[at].at[mine], send_sem.at[c], recv_sem.at[c]))
    norm_loads = (
        pltpu.make_async_copy(slope_norm, norms.at[pl.ds(me, 1)], norm_in.at[0]),
        pltpu.make_async_copy(param_norm, norm_own, norm_in.at[1]),
    )
    norm_sends = [
        remote(slope_norm, norms.at[pl.ds(me, 1)], norm_send.at[0], norm_recv.at[0]),
        remote(param_norm, norm_got, norm_send.at[1], norm_recv.at[1]),
    ]

    for fetch in fetches:
        fetch.start()
    barrier = pltpu.get_barrier_semaphore()
    pl.semaphore_signal(barrier, inc=1, device_id=there, device_id_type=pl.DeviceIdType.MESH)
    for load in loads:
        load[0].start()
        load[1].start()
    for load in norm_loads:
        load.start()
    pl.semaphore_wait(barrier, 1)
    for send in norm_sends:
        send.start()

    for c, (at, start, rows) in enumerate(chunks):
        fetches[c].wait()
        step = block(rows, kept[at].shape[1], size)

        @pl.loop(0, rows // step)
        def encode(turn, at=at, start=start, step=step):
            span = pl.ds(pl.multiple_of(start + turn * step, 16), step)
            code[at][span] = coded(away[at][span])

        sends[c].start()

    backs = []
    for c, (at, start, rows) in enumerate(chunks):
        loads[c][0].wait()
        loads[c][1].wait()
        sends[c].wait_recv()
        step = block(rows, kept[at].shape[1], size)

        @pl.loop(0, rows // step)
        def update(turn, at=at, start=start, step=step):
            first = pl.multiple_of(start + turn * step, 16)
            span = pl.ds(first, step)
            total = own[at][span] + decoded(got[at][span])
            moved = kept[at][span] - (learn_rate * rate) * total
            kept[at][span] = moved
            halfs[at][half_of(at, me, first, step)] = moved.astype(jnp.bfloat16)

        place = half_of(at, me, start, rows)
        back = remote(halfs[at].at[place], halfs[at].at[place], back_send.at[c], back_recv.at[c])
        back.start()
        backs.append(back)

    for load in norm_loads:
        load.wait()
    for send in norm_sends:
        send.wait_recv()
    width = norm_own.shape[0]
    total = norms[0:1] + norms[1:2]
    for where, held in ((me, norm_own), (peer, norm_got)):
        cut = pl.ds(pl.multiple_of(where * width, width), width)
        norm_all[0:1, cut] = held[...].reshape(1, width)
    moved = norm_all[...] - learn_rate * (total * rate)
    norm_all[...] = moved
    norm_half[...] = moved.reshape(n * width).astype(jnp.bfloat16)
    cut = pl.ds(pl.multiple_of(me * width, width), width)
    norm_next[...] = norm_all[0:1, cut].reshape(width)

    for send in sends + norm_sends:
        send.wait_send()
    for back in backs:
        back.wait()


def settle(count, *refs):
    sems = refs[-1]
    copies = [
        pltpu.make_async_copy(refs[k], refs[count + k], sems.at[k]) for k in range(count)
    ]
    for copy in copies:
        copy.start()
    for copy in copies:
        copy.wait()


def shards(n, *arrays):
    m = len(arrays) // 2 - 1
    slopes, slope_norm = list(arrays[:m]), arrays[m]
    params, param_norm = list(arrays[m + 1 : -1]), arrays[-1]
    turned = [2, 3, 4]
    by_row = [slope.shape[1] != param.shape[0] for slope, param in zip(slopes, params)]
    for at in turned:
        slopes[at] = slopes[at].transpose(0, 2, 1)
        params[at] = params[at].T
        by_row[at] = not by_row[at]
    f32, bf16 = jnp.float32, jnp.bfloat16
    halves = [param.shape for param in params]
    wholes = [slope.shape[1:] for slope in slopes]
    small = min(half[0] * half[1] for half in halves)
    chunks = plan(halves, small)
    count = len(chunks)
    width = param_norm.shape[0]
    dma = pltpu.SemaphoreType.DMA
    results = sum(rows * columns for rows, columns in wholes) * 2
    results += sum(rows * columns for rows, columns in halves) * 4
    outs = pl.pallas_call(
        functools.partial(exchange, n, by_row, chunks, small // 2, n ** (-0.5)),
        out_shape=(
            *[pltpu.VMEM(whole, bf16) for whole in wholes],
            pltpu.VMEM((n * width,), bf16),
            *[pltpu.VMEM(half, f32) for half in halves],
            pltpu.VMEM((width,), f32),
        ),
        in_specs=[ANY] * (2 * m + 2),
        out_specs=[pl.BlockSpec(memory_space=pltpu.VMEM)] * (2 * m + 2),
        scratch_shapes=[
            *[pltpu.VMEM(half, f32) for half in halves * 2],
            *[pltpu.VMEM(half, bf16) for half in halves * 2],
            pltpu.VMEM((n, n * width), f32),
            pltpu.VMEM((width,), f32),
            pltpu.VMEM((width,), f32),
            pltpu.VMEM((1, n * width), f32),
            *[dma((count,))] * 7,
            *[dma((2,))] * 3,
        ],
        compiler_params=pltpu.CompilerParams(
            collective_id=0, has_side_effects=True, vmem_limit_bytes=VMEM_BYTES - results - 192 * 1024
        ),
        name="exchange",
    )(*slopes, slope_norm, *params, param_norm)
    outs = list(pl.pallas_call(
        functools.partial(settle, len(outs)),
        out_shape=[jax.ShapeDtypeStruct(out.shape, out.dtype) for out in outs],
        in_specs=[pl.BlockSpec(memory_space=pltpu.VMEM)] * len(outs),
        out_specs=[ANY] * len(outs),
        scratch_shapes=[dma((len(outs),))],
        compiler_params=pltpu.CompilerParams(vmem_limit_bytes=2 * 1024 * 1024),
        name="settle",
    )(*outs))
    for at in turned:
        outs[at] = outs[at].T
        outs[m + 1 + at] = outs[m + 1 + at].T
    return tuple(outs)


def spread(
    slope_up,
    slope_down,
    slope_query,
    slope_key,
    slope_value,
    slope_mixed,
    slope_norm,
    param_up,
    param_down,
    param_query,
    param_key,
    param_value,
    param_mixed,
    param_norm,
):
    mean_up, mean_down, mean_query, mean_key, mean_value, mean_mixed = (
        lax.psum_scatter(slope_up[0], "replica", scatter_dimension=0, tiled=True),
        lax.psum_scatter(slope_down[0], "replica", scatter_dimension=1, tiled=True),
        lax.psum_scatter(slope_query[0], "replica", scatter_dimension=0, tiled=True),
        lax.psum_scatter(slope_key[0], "replica", scatter_dimension=0, tiled=True),
        lax.psum_scatter(slope_value[0], "replica", scatter_dimension=0, tiled=True),
        lax.psum_scatter(slope_mixed[0], "replica", scatter_dimension=1, tiled=True),
    )
    whole_norm = lax.psum(slope_norm[0], "replica")
    place = lax.axis_index("replica")
    mean_norm = lax.dynamic_slice_in_dim(
        whole_norm, place * param_norm.shape[0], param_norm.shape[0]
    )
    mean_rate = lax.axis_size("replica") ** (-0.5)
    mean_up = mean_up * mean_rate
    mean_down = mean_down * mean_rate
    mean_query = mean_query * mean_rate
    mean_key = mean_key * mean_rate
    mean_value = mean_value * mean_rate
    mean_mixed = mean_mixed * mean_rate
    mean_norm = mean_norm * mean_rate
    next_up = param_up - learn_rate * mean_up
    next_down = param_down - learn_rate * mean_down
    next_query = param_query - learn_rate * mean_query
    next_key = param_key - learn_rate * mean_key
    next_value = param_value - learn_rate * mean_value
    next_mixed = param_mixed - learn_rate * mean_mixed
    next_norm = param_norm - learn_rate * mean_norm
    half_up, half_down, half_query, half_key, half_value, half_mixed, half_norm = (
        lax.all_gather(next_up.astype(jnp.bfloat16), "replica", axis=0, tiled=True),
        lax.all_gather(next_down.astype(jnp.bfloat16), "replica", axis=1, tiled=True),
        lax.all_gather(next_query.astype(jnp.bfloat16), "replica", axis=0, tiled=True),
        lax.all_gather(next_key.astype(jnp.bfloat16), "replica", axis=0, tiled=True),
        lax.all_gather(next_value.astype(jnp.bfloat16), "replica", axis=0, tiled=True),
        lax.all_gather(next_mixed.astype(jnp.bfloat16), "replica", axis=1, tiled=True),
        lax.all_gather(next_norm.astype(jnp.bfloat16), "replica", axis=0, tiled=True),
    )
    return (
        half_up,
        half_down,
        half_query,
        half_key,
        half_value,
        half_mixed,
        half_norm,
        next_up,
        next_down,
        next_query,
        next_key,
        next_value,
        next_mixed,
        next_norm,
    )


def solution(mesh):
    placed = (
        P(("unit", "replica"), None, "model"),
        P(("unit", "replica"), "model", None),
        P(("unit", "replica"), None, "model"),
        P(("unit", "replica"), None, "model"),
        P(("unit", "replica"), None, "model"),
        P(("unit", "replica"), "model", None),
        P(("unit", "replica"), None),
        P(("unit", "replica"), "model"),
        P(("unit", "model"), "replica"),
        P(("unit", "replica"), "model"),
        P(("unit", "replica"), "model"),
        P(("unit", "replica"), "model"),
        P(("unit", "model"), "replica"),
        P(("unit", "replica")),
    )
    n = mesh.shape["replica"]
    return jax.shard_map(
        functools.partial(shards, n) if n == 2 else spread,
        mesh=mesh,
        in_specs=placed,
        out_specs=(
            P("unit", "model"),
            P(("unit", "model"), None),
            P("unit", "model"),
            P("unit", "model"),
            P("unit", "model"),
            P(("unit", "model"), None),
            P("unit"),
            P(("unit", "replica"), "model"),
            P(("unit", "model"), "replica"),
            P(("unit", "replica"), "model"),
            P(("unit", "replica"), "model"),
            P(("unit", "replica"), "model"),
            P(("unit", "model"), "replica"),
            P(("unit", "replica")),
        ),
        check_vma=False,
    )
```

```python
import functools

import jax
import jax.numpy as jnp
from jax import lax
from jax.experimental import pallas as pl
from jax.experimental.pallas import tpu as pltpu
from jax.sharding import PartitionSpec as P

learn_rate = 0.3
LOG2E = 1.4426950408889634
ANY = pl.BlockSpec(memory_space=pl.ANY)
VMEM_BYTES = 67043328
ROOM = 1280 * 1024


def plan(halves, order, size):
    chunks = []
    for at in order:
        rows, columns = halves[at]
        parts = max(1, rows * columns // size)
        if rows % (16 * parts):
            parts = 1
        chunks += [(at, part * (rows // parts), rows // parts) for part in range(parts)]
    return chunks


def block(rows, columns, size):
    step = rows
    while step % 32 == 0 and step * columns > size:
        step //= 2
    return step


def coded(slope):
    scaled = slope * 256.0
    square = scaled * scaled
    fourth = square * square
    eighth = fourth * fourth
    size = jnp.maximum(eighth, eighth * eighth)
    return jnp.where(slope < 0.0, -size, size).astype(jnp.bfloat16)


def decoded(code):
    code = code.astype(jnp.float32)
    power = jnp.log(jnp.abs(code))
    size = jnp.exp2(jnp.minimum(power * (LOG2E / 8), power * (LOG2E / 16)) - 8.0)
    return jnp.where(code < 0.0, -size, size)


def exchange(n, by_row, spots, chunks, size, rate, *refs):
    m = len(by_row)
    slopes, slope_norm = refs[:m], refs[m]
    params, param_norm = refs[m + 1 : 2 * m + 1], refs[2 * m + 1]
    refs = refs[2 * m + 2 :]
    direct = [at for at in range(m) if at not in spots]
    packed, halfs, norm_half = refs[0], dict(zip(direct, refs[1:])), refs[len(direct) + 1]
    refs = refs[len(direct) + 2 :]
    kept, norm_next = refs[:m], refs[m]
    refs = refs[m + 1 :]
    own, away, code, got = refs[:m], refs[m : 2 * m], refs[2 * m : 3 * m], refs[3 * m : 4 * m]
    norms, norm_own, norm_got, norm_all, away_sem, recv_sem, own_sem, all_sem, norm_sem = refs[4 * m :]

    me = lax.axis_index("replica")
    peer = 1 - me
    there = {"replica": peer}

    def half_of(at, who, start, rows):
        height, width = kept[at].shape
        if by_row[at]:
            return pl.ds(pl.multiple_of(who * height + start, 16), rows), pl.ds(0, width)
        return pl.ds(start, rows), pl.ds(pl.multiple_of(who * width, width), width)

    def remote(source, target, out_sem, in_sem):
        return pltpu.make_async_remote_copy(
            src_ref=source,
            dst_ref=target,
            send_sem=out_sem,
            recv_sem=in_sem,
            device_id=there,
            device_id_type=pl.DeviceIdType.MESH,
        )

    def drain(sem, size):
        part = slopes[0].at[0, pl.ds(0, size // (4 * slopes[0].shape[2]))]
        pltpu.make_async_copy(part, part, sem).wait()

    fetches, loads, sends = [], {}, []
    for c, (at, start, rows) in enumerate(chunks):
        mine = pl.ds(start, rows)
        fetches.append(pltpu.make_async_copy(
            slopes[at].at[(0, *half_of(at, peer, start, rows))], away[at].at[mine], away_sem.at[c]
        ))
        sends.append(remote(code[at].at[mine], got[at].at[mine], all_sem.at[0], recv_sem.at[c]))
    for at in dict.fromkeys(at for at, _, _ in chunks):
        height = kept[at].shape[0]
        loads[at] = (
            pltpu.make_async_copy(
                slopes[at].at[(0, *half_of(at, me, 0, height))], own[at], own_sem.at[at]
            ),
            pltpu.make_async_copy(params[at], kept[at], own_sem.at[at]),
        )
    norm_loads = (
        pltpu.make_async_copy(slope_norm, norms.at[pl.ds(me, 1)], norm_sem.at[0]),
        pltpu.make_async_copy(param_norm, norm_own, norm_sem.at[1]),
    )
    norm_sends = [
        remote(slope_norm, norms.at[pl.ds(me, 1)], norm_sem.at[2], norm_sem.at[3]),
        remote(param_norm, norm_got, norm_sem.at[4], norm_sem.at[5]),
    ]

    count = len(chunks)
    for fetch in fetches:
        fetch.start()
    barrier = pltpu.get_barrier_semaphore()
    pl.semaphore_signal(barrier, inc=1, device_id=there, device_id_type=pl.DeviceIdType.MESH)
    for load in loads.values():
        load[0].start()
        load[1].start()
    for load in norm_loads:
        load.start()
    pl.semaphore_wait(barrier, 1)
    for send in norm_sends:
        send.start()

    def encode(c):
        at, start, rows = chunks[c]
        fetches[c].wait()
        step = block(rows, kept[at].shape[1], size)

        @pl.loop(0, rows // step)
        def turns(turn):
            span = pl.ds(pl.multiple_of(start + turn * step, 16), step)
            code[at][span] = coded(away[at][span])

        sends[c].start()

    def update(c):
        at, start, rows = chunks[c]
        if start == 0:
            drain(own_sem.at[at], 8 * kept[at].shape[0] * kept[at].shape[1])
        sends[c].wait_recv()
        width = kept[at].shape[1]
        step = block(rows, width, size)
        top, fold, columns = spots.get(at, (0, rows, 0))

        @pl.loop(0, rows // step)
        def turns(turn):
            first = pl.multiple_of(start + turn * step, 16)
            span = pl.ds(first, step)
            total = own[at][span] + decoded(got[at][span])
            moved = kept[at][span] - (learn_rate * rate) * total
            kept[at][span] = moved
            if at in spots:
                row = pl.multiple_of(top + lax.rem(first, fold), 16)
                column = pl.multiple_of(lax.div(first, fold) * columns, 128)
                packed[pl.ds(row, step), pl.ds(column, width)] = moved.astype(jnp.bfloat16)
            else:
                halfs[at][half_of(at, me, first, step)] = moved.astype(jnp.bfloat16)

        if at in spots:
            return
        place = half_of(at, me, start, rows)
        back = remote(halfs[at].at[place], halfs[at].at[place], all_sem.at[1], all_sem.at[2])
        back.start()

    for c in range(len(chunks)):
        encode(c)
    for c in range(len(chunks)):
        update(c)

    for load in norm_loads:
        load.wait()
    for send in norm_sends:
        send.wait_recv()
    width = norm_own.shape[0]
    total = norms[0:1] + norms[1:2]
    for where, held in ((me, norm_own), (peer, norm_got)):
        cut = pl.ds(pl.multiple_of(where * width, width), width)
        norm_all[0:1, cut] = held[...].reshape(1, width)
    moved = norm_all[...] - learn_rate * (total * rate)
    norm_all[...] = moved
    norm_half[...] = moved.reshape(n * width).astype(jnp.bfloat16)
    cut = pl.ds(pl.multiple_of(me * width, width), width)
    norm_next[...] = norm_all[0:1, cut].reshape(width)

    for send in norm_sends:
        send.wait_send()
    sizes = [2 * half.shape[0] * half.shape[1] for half in kept]
    drain(all_sem.at[0], sum(sizes))
    back = sum(sizes[at] for at in range(m) if at not in spots)
    drain(all_sem.at[1], back)
    drain(all_sem.at[2], back)


def half_at(by_row, who, shape, start, rows):
    height, width = shape
    if by_row:
        return pl.ds(pl.multiple_of(who * height + start, 16), rows), pl.ds(0, width)
    return pl.ds(start, rows), pl.ds(pl.multiple_of(who * width, width), width)


def pack(halves, later):
    width = max(halves[at][1] for at in later)
    spots, top = {}, 0
    for at in later:
        rows, columns = halves[at]
        spots[at] = (top, rows * columns // width, columns)
        top += spots[at][1]
    return spots, (top, width)


def unpacked(packed, target, by_row, who, shape, place):
    top, rows, columns = place
    return [
        (
            packed.at[pl.ds(top, rows), pl.ds(start // rows * columns, columns)],
            target.at[half_at(by_row, who, shape, start, rows)],
        )
        for start in range(0, shape[0], rows)
    ]


def settle(by_row, shapes, spots, *refs):
    m = len(by_row)
    count = 2 * m + 2
    packed, ready, outs, sems = refs[0], refs[1 : -1 - count], refs[-1 - count : -1], refs[-1]
    me = lax.axis_index("replica")
    plain = [out for k, out in enumerate(outs) if k not in spots]
    copies = [
        pltpu.make_async_copy(source, target, sems.at[1 + k])
        for k, (source, target) in enumerate(zip(ready, plain))
    ]
    for at in spots:
        for pair in unpacked(packed, outs[at], by_row[at], me, shapes[at], spots[at]):
            pltpu.make_async_copy(*pair, sems.at[0]).start()
    for copy in copies:
        copy.start()
    for copy in copies:
        copy.wait()
    pltpu.make_async_copy(packed, packed, sems.at[0]).wait()


def finish(by_row, shapes, spots, *refs):
    packed, outs, sem = refs[0], refs[-1 - len(spots) : -1], refs[-1]
    peer = 1 - lax.axis_index("replica")
    for out, at in zip(outs, spots):
        for pair in unpacked(packed, out, by_row[at], peer, shapes[at], spots[at]):
            pltpu.make_async_copy(*pair, sem).start()
    pltpu.make_async_copy(packed, packed, sem).wait()


def shards(n, *arrays):
    m = len(arrays) // 2 - 1
    slopes, slope_norm = list(arrays[:m]), arrays[m]
    params, param_norm = list(arrays[m + 1 : -1]), arrays[-1]
    turned = [2, 3, 4]
    by_row = [slope.shape[1] != param.shape[0] for slope, param in zip(slopes, params)]
    for at in turned:
        slopes[at] = slopes[at].transpose(0, 2, 1)
        params[at] = params[at].T
        by_row[at] = not by_row[at]
    f32, bf16 = jnp.float32, jnp.bfloat16
    halves = [param.shape for param in params]
    wholes = [slope.shape[1:] for slope in slopes]
    small = min(half[0] * half[1] for half in halves)
    later = [0,1,5]
    order = [2, 3, 4, 5, 0, 1]
    spots, packed = pack(halves, later)
    chunks = plan(halves, order, 2*small)
    count = len(chunks)
    width = param_norm.shape[0]
    dma = pltpu.SemaphoreType.DMA
    direct = [wholes[at] for at in range(m) if at not in spots]
    results = sum(rows * columns for rows, columns in direct + [packed]) * 2
    results += sum(rows * columns for rows, columns in halves) * 4
    kept = pl.pallas_call(
        functools.partial(exchange, n, by_row, spots, chunks, small // 2, n ** (-0.5)),
        out_shape=(
            pltpu.VMEM(packed, bf16),
            *[pltpu.VMEM(whole, bf16) for whole in direct],
            pltpu.VMEM((n * width,), bf16),
            *[pltpu.VMEM(half, f32) for half in halves],
            pltpu.VMEM((width,), f32),
        ),
        in_specs=[ANY] * (2 * m + 2),
        out_specs=[pl.BlockSpec(memory_space=pltpu.VMEM)] * (len(direct) + m + 3),
        scratch_shapes=[
            *[pltpu.VMEM(half, f32) for half in halves * 2],
            *[pltpu.VMEM(half, bf16) for half in halves * 2],
            pltpu.VMEM((n, n * width), f32),
            pltpu.VMEM((width,), f32),
            pltpu.VMEM((width,), f32),
            pltpu.VMEM((1, n * width), f32),
            *[dma((count,))] * 2,
            dma((m,)),
            dma((3,)),
            dma((6,)),
        ],
        compiler_params=pltpu.CompilerParams(
            collective_id=0, has_side_effects=True, vmem_limit_bytes=VMEM_BYTES - results - ROOM
        ),
        name="exchange",
    )(*slopes, slope_norm, *params, param_norm)
    swap = [(who, n - 1 - who) for who in range(n)]
    theirs = lax.ppermute(kept[0], "replica", swap)
    shapes = wholes + [(n * width,)] + halves + [(width,)]
    types = [bf16] * (m + 1) + [f32] * (m + 1)
    small_grant = pltpu.CompilerParams(vmem_limit_bytes=2 * 1024 * 1024)
    outs = list(pl.pallas_call(
        functools.partial(settle, by_row, halves, spots),
        out_shape=[jax.ShapeDtypeStruct(*out) for out in zip(shapes, types)],
        in_specs=[pl.BlockSpec(memory_space=pltpu.VMEM)] * len(kept),
        out_specs=[ANY] * len(shapes),
        scratch_shapes=[dma((len(kept),))],
        compiler_params=small_grant,
        cost_estimate=pl.CostEstimate(flops=10**8, bytes_accessed=results, transcendentals=0),
        name="settle",
    )(*kept))
    done = pl.pallas_call(
        functools.partial(finish, by_row, halves, spots),
        out_shape=[jax.ShapeDtypeStruct(outs[at].shape, outs[at].dtype) for at in spots],
        in_specs=[pl.BlockSpec(memory_space=pltpu.VMEM)] + [ANY] * len(spots),
        out_specs=[ANY] * len(spots),
        scratch_shapes=[dma(())],
        input_output_aliases={1 + k: k for k in range(len(spots))},
        compiler_params=small_grant,
        name="finish",
    )(theirs, *[outs[at] for at in spots])
    for at, whole in zip(spots, done):
        outs[at] = whole
    for at in turned:
        outs[at] = outs[at].T
        outs[m + 1 + at] = outs[m + 1 + at].T
    return tuple(outs)


def spread(
    slope_up,
    slope_down,
    slope_query,
    slope_key,
    slope_value,
    slope_mixed,
    slope_norm,
    param_up,
    param_down,
    param_query,
    param_key,
    param_value,
    param_mixed,
    param_norm,
):
    mean_up, mean_down, mean_query, mean_key, mean_value, mean_mixed = (
        lax.psum_scatter(slope_up[0], "replica", scatter_dimension=0, tiled=True),
        lax.psum_scatter(slope_down[0], "replica", scatter_dimension=1, tiled=True),
        lax.psum_scatter(slope_query[0], "replica", scatter_dimension=0, tiled=True),
        lax.psum_scatter(slope_key[0], "replica", scatter_dimension=0, tiled=True),
        lax.psum_scatter(slope_value[0], "replica", scatter_dimension=0, tiled=True),
        lax.psum_scatter(slope_mixed[0], "replica", scatter_dimension=1, tiled=True),
    )
    whole_norm = lax.psum(slope_norm[0], "replica")
    place = lax.axis_index("replica")
    mean_norm = lax.dynamic_slice_in_dim(
        whole_norm, place * param_norm.shape[0], param_norm.shape[0]
    )
    mean_rate = lax.axis_size("replica") ** (-0.5)
    mean_up = mean_up * mean_rate
    mean_down = mean_down * mean_rate
    mean_query = mean_query * mean_rate
    mean_key = mean_key * mean_rate
    mean_value = mean_value * mean_rate
    mean_mixed = mean_mixed * mean_rate
    mean_norm = mean_norm * mean_rate
    next_up = param_up - learn_rate * mean_up
    next_down = param_down - learn_rate * mean_down
    next_query = param_query - learn_rate * mean_query
    next_key = param_key - learn_rate * mean_key
    next_value = param_value - learn_rate * mean_value
    next_mixed = param_mixed - learn_rate * mean_mixed
    next_norm = param_norm - learn_rate * mean_norm
    half_up, half_down, half_query, half_key, half_value, half_mixed, half_norm = (
        lax.all_gather(next_up.astype(jnp.bfloat16), "replica", axis=0, tiled=True),
        lax.all_gather(next_down.astype(jnp.bfloat16), "replica", axis=1, tiled=True),
        lax.all_gather(next_query.astype(jnp.bfloat16), "replica", axis=0, tiled=True),
        lax.all_gather(next_key.astype(jnp.bfloat16), "replica", axis=0, tiled=True),
        lax.all_gather(next_value.astype(jnp.bfloat16), "replica", axis=0, tiled=True),
        lax.all_gather(next_mixed.astype(jnp.bfloat16), "replica", axis=1, tiled=True),
        lax.all_gather(next_norm.astype(jnp.bfloat16), "replica", axis=0, tiled=True),
    )
    return (
        half_up,
        half_down,
        half_query,
        half_key,
        half_value,
        half_mixed,
        half_norm,
        next_up,
        next_down,
        next_query,
        next_key,
        next_value,
        next_mixed,
        next_norm,
    )


def solution(mesh):
    placed = (
        P(("unit", "replica"), None, "model"),
        P(("unit", "replica"), "model", None),
        P(("unit", "replica"), None, "model"),
        P(("unit", "replica"), None, "model"),
        P(("unit", "replica"), None, "model"),
        P(("unit", "replica"), "model", None),
        P(("unit", "replica"), None),
        P(("unit", "replica"), "model"),
        P(("unit", "model"), "replica"),
        P(("unit", "replica"), "model"),
        P(("unit", "replica"), "model"),
        P(("unit", "replica"), "model"),
        P(("unit", "model"), "replica"),
        P(("unit", "replica")),
    )
    n = mesh.shape["replica"]
    return jax.shard_map(
        functools.partial(shards, n) if n == 2 else spread,
        mesh=mesh,
        in_specs=placed,
        out_specs=(
            P("unit", "model"),
            P(("unit", "model"), None),
            P("unit", "model"),
            P("unit", "model"),
            P("unit", "model"),
            P(("unit", "model"), None),
            P("unit"),
            P(("unit", "replica"), "model"),
            P(("unit", "model"), "replica"),
            P(("unit", "replica"), "model"),
            P(("unit", "replica"), "model"),
            P(("unit", "replica"), "model"),
            P(("unit", "model"), "replica"),
            P(("unit", "replica")),
        ),
        check_vma=False,
    )
```

```python
import functools

import jax
import jax.numpy as jnp
from jax import lax
from jax.experimental import pallas as pl
from jax.experimental.pallas import tpu as pltpu
from jax.sharding import PartitionSpec as P

learn_rate = 0.3
LOG2E = 1.4426950408889634
ANY = pl.BlockSpec(memory_space=pl.ANY)
VMEM_BYTES = 67043328
ROOM = 1280 * 1024


def plan(halves, order, size):
    chunks = []
    for at in order:
        rows, columns = halves[at]
        parts = 2 if at == order[0] else max(1, rows * columns // size)
        if rows % (16 * parts):
            parts = 1
        chunks += [(at, part * (rows // parts), rows // parts) for part in range(parts)]
    return chunks


def block(rows, columns, size):
    step = rows
    while step % 32 == 0 and step * columns > size:
        step //= 2
    return step


def coded(slope):
    scaled = slope * 256.0
    square = scaled * scaled
    fourth = square * square
    eighth = fourth * fourth
    size = jnp.maximum(eighth, eighth * eighth)
    return jnp.where(slope < 0.0, -size, size).astype(jnp.bfloat16)


def decoded(code):
    code = code.astype(jnp.float32)
    power = jnp.log(jnp.abs(code))
    size = jnp.exp2(jnp.minimum(power * (LOG2E / 8), power * (LOG2E / 16)) - 8.0)
    return jnp.where(code < 0.0, -size, size)


def exchange(n, by_row, spots, chunks, size, rate, *refs):
    m = len(by_row)
    slopes, slope_norm = refs[:m], refs[m]
    params, param_norm = refs[m + 1 : 2 * m + 1], refs[2 * m + 1]
    refs = refs[2 * m + 2 :]
    direct = [at for at in range(m) if at not in spots]
    packed, halfs, norm_half = refs[0], dict(zip(direct, refs[1:])), refs[len(direct) + 1]
    refs = refs[len(direct) + 2 :]
    kept, norm_next = refs[:m], refs[m]
    refs = refs[m + 1 :]
    own, away, code, got = refs[:m], refs[m : 2 * m], refs[2 * m : 3 * m], refs[3 * m : 4 * m]
    norms, norm_own, norm_got, norm_all, away_sem, recv_sem, own_sem, all_sem, norm_sem = refs[4 * m :]

    me = lax.axis_index("replica")
    peer = 1 - me
    there = {"replica": peer}

    def half_of(at, who, start, rows):
        height, width = kept[at].shape
        if by_row[at]:
            return pl.ds(pl.multiple_of(who * height + start, 16), rows), pl.ds(0, width)
        return pl.ds(start, rows), pl.ds(pl.multiple_of(who * width, width), width)

    def remote(source, target, out_sem, in_sem):
        return pltpu.make_async_remote_copy(
            src_ref=source,
            dst_ref=target,
            send_sem=out_sem,
            recv_sem=in_sem,
            device_id=there,
            device_id_type=pl.DeviceIdType.MESH,
        )

    def drain(sem, size):
        part = slopes[0].at[0, pl.ds(0, size // (4 * slopes[0].shape[2]))]
        pltpu.make_async_copy(part, part, sem).wait()

    sizes = [half.shape[0] * half.shape[1] for half in kept]
    least = min(sizes)
    big = [at for at in range(m) if sizes[at] > least]
    group = [1 + big.index(at) if at in big else 0 for at in range(m)]
    fetches, loads, sends = [], {}, []
    for c, (at, start, rows) in enumerate(chunks):
        mine = pl.ds(start, rows)
        fetches.append(pltpu.make_async_copy(
            slopes[at].at[(0, *half_of(at, peer, start, rows))], away[at].at[mine], away_sem.at[c]
        ))
        sends.append(remote(code[at].at[mine], got[at].at[mine], all_sem.at[0], recv_sem.at[c]))
    for at in dict.fromkeys(at for at, _, _ in chunks):
        height = kept[at].shape[0]
        loads[at] = (
            pltpu.make_async_copy(
                slopes[at].at[(0, *half_of(at, me, 0, height))], own[at], own_sem.at[group[at]]
            ),
            pltpu.make_async_copy(params[at], kept[at], own_sem.at[group[at]]),
        )
    norm_loads = (
        pltpu.make_async_copy(slope_norm, norms.at[pl.ds(me, 1)], norm_sem.at[0]),
        pltpu.make_async_copy(param_norm, norm_own, norm_sem.at[1]),
    )
    norm_sends = [
        remote(slope_norm, norms.at[pl.ds(me, 1)], norm_sem.at[2], norm_sem.at[3]),
        remote(param_norm, norm_got, norm_sem.at[4], norm_sem.at[5]),
    ]

    for fetch in fetches:
        fetch.start()
    barrier = pltpu.get_barrier_semaphore()
    pl.semaphore_signal(barrier, inc=1, device_id=there, device_id_type=pl.DeviceIdType.MESH)
    for load in loads.values():
        load[0].start()
        load[1].start()
    for load in norm_loads:
        load.start()
    pl.semaphore_wait(barrier, 1)
    for send in norm_sends:
        send.start()

    def encode(c):
        at, start, rows = chunks[c]
        fetches[c].wait()
        step = block(rows, kept[at].shape[1], size)

        @pl.loop(0, rows // step)
        def turns(turn):
            span = pl.ds(pl.multiple_of(start + turn * step, 16), step)
            code[at][span] = coded(away[at][span])

        sends[c].start()

    def update(c):
        at, start, rows = chunks[c]
        if group[at] not in ready:
            ready.add(group[at])
            drain(own_sem.at[group[at]], 8 * sum(sizes[k] for k in range(m) if group[k] == group[at]))
        sends[c].wait_recv()
        width = kept[at].shape[1]
        step = block(rows, width, size)
        top, fold, columns = spots.get(at, (0, rows, 0))

        @pl.loop(0, rows // step)
        def turns(turn):
            first = pl.multiple_of(start + turn * step, 16)
            span = pl.ds(first, step)
            total = own[at][span] + decoded(got[at][span])
            moved = kept[at][span] - (learn_rate * rate) * total
            kept[at][span] = moved
            if at in spots:
                row = pl.multiple_of(top + lax.rem(first, fold), 16)
                column = pl.multiple_of(lax.div(first, fold) * columns, 128)
                packed[pl.ds(row, step), pl.ds(column, width)] = moved.astype(jnp.bfloat16)
            else:
                halfs[at][half_of(at, me, first, step)] = moved.astype(jnp.bfloat16)

        if at in spots:
            return
        place = half_of(at, me, start, rows)
        back = remote(halfs[at].at[place], halfs[at].at[place], all_sem.at[0], all_sem.at[1])
        back.start()

    ready = set()
    for c in range(len(chunks)):
        encode(c)
    for c in range(len(chunks)):
        update(c)

    for load in norm_loads:
        load.wait()
    for send in norm_sends:
        send.wait_recv()
    width = norm_own.shape[0]
    total = norms[0:1] + norms[1:2]
    for where, held in ((me, norm_own), (peer, norm_got)):
        cut = pl.ds(pl.multiple_of(where * width, width), width)
        norm_all[0:1, cut] = held[...].reshape(1, width)
    moved = norm_all[...] - learn_rate * (total * rate)
    norm_all[...] = moved
    norm_half[...] = moved.reshape(n * width).astype(jnp.bfloat16)
    cut = pl.ds(pl.multiple_of(me * width, width), width)
    norm_next[...] = norm_all[0:1, cut].reshape(width)

    for send in norm_sends:
        send.wait_send()
    back = 2 * sum(sizes[at] for at in range(m) if at not in spots)
    drain(all_sem.at[0], 2 * sum(sizes) + back)
    drain(all_sem.at[1], back)


def half_at(by_row, who, shape, start, rows):
    height, width = shape
    if by_row:
        return pl.ds(pl.multiple_of(who * height + start, 16), rows), pl.ds(0, width)
    return pl.ds(start, rows), pl.ds(pl.multiple_of(who * width, width), width)


def pack(halves, later):
    width = max(halves[at][1] for at in later)
    spots, top = {}, 0
    for at in later:
        rows, columns = halves[at]
        spots[at] = (top, rows * columns // width, columns)
        top += spots[at][1]
    return spots, (top, width)


def unpacked(packed, target, by_row, who, shape, place):
    top, rows, columns = place
    return [
        (
            packed.at[pl.ds(top, rows), pl.ds(start // rows * columns, columns)],
            target.at[half_at(by_row, who, shape, start, rows)],
        )
        for start in range(0, shape[0], rows)
    ]


def settle(by_row, shapes, spots, *refs):
    m = len(by_row)
    count = 2 * m + 2
    packed, ready, outs, sems = refs[0], refs[1 : -1 - count], refs[-1 - count : -1], refs[-1]
    me = lax.axis_index("replica")
    plain = [out for k, out in enumerate(outs) if k not in spots]
    pairs = {None: []}
    for at in spots:
        pairs[None] += unpacked(packed, outs[at], by_row[at], me, shapes[at], spots[at])
    for pair in zip(ready, plain):
        shape = pair[0].shape
        key = (shape, str(pair[0].dtype)) if len(shape) == 2 else shape
        pairs.setdefault(key, []).append(pair)
    for k, same in enumerate(pairs.values()):
        for pair in same:
            pltpu.make_async_copy(*pair, sems.at[k]).start()
    for k, same in enumerate(pairs.values()):
        source, target = same[0]
        if len(same) > 1:
            size = sum(source.size * source.dtype.itemsize for source, _ in same)
            source = target = packed.at[pl.ds(0, size // (2 * packed.shape[1]))]
        pltpu.make_async_copy(source, target, sems.at[k]).wait()


def finish(by_row, shapes, spots, *refs):
    packed, outs, sem = refs[0], refs[-1 - len(spots) : -1], refs[-1]
    peer = 1 - lax.axis_index("replica")
    for out, at in zip(outs, spots):
        for pair in unpacked(packed, out, by_row[at], peer, shapes[at], spots[at]):
            pltpu.make_async_copy(*pair, sem).start()
    pltpu.make_async_copy(packed, packed, sem).wait()


def shards(n, *arrays):
    m = len(arrays) // 2 - 1
    slopes, slope_norm = list(arrays[:m]), arrays[m]
    params, param_norm = list(arrays[m + 1 : -1]), arrays[-1]
    turned = [2, 3, 4]
    by_row = [slope.shape[1] != param.shape[0] for slope, param in zip(slopes, params)]
    for at in turned:
        slopes[at] = slopes[at].transpose(0, 2, 1)
        params[at] = params[at].T
        by_row[at] = not by_row[at]
    f32, bf16 = jnp.float32, jnp.bfloat16
    halves = [param.shape for param in params]
    wholes = [slope.shape[1:] for slope in slopes]
    small = min(half[0] * half[1] for half in halves)
    later = [0, 1, 5]
    smalls = sum(half[0] * half[1] == small for half in halves)
    order = [2, 3, 4, 5, 0, 1]
    spots, packed = pack(halves, later)
    chunks = plan(halves, order, 2*small)
    count = len(chunks)
    width = param_norm.shape[0]
    dma = pltpu.SemaphoreType.DMA
    direct = [wholes[at] for at in range(m) if at not in spots]
    results = sum(rows * columns for rows, columns in direct + [packed]) * 2
    results += sum(rows * columns for rows, columns in halves) * 4
    kept = pl.pallas_call(
        functools.partial(exchange, n, by_row, spots, chunks, small // 2, n ** (-0.5)),
        out_shape=(
            pltpu.VMEM(packed, bf16),
            *[pltpu.VMEM(whole, bf16) for whole in direct],
            pltpu.VMEM((n * width,), bf16),
            *[pltpu.VMEM(half, f32) for half in halves],
            pltpu.VMEM((width,), f32),
        ),
        in_specs=[ANY] * (2 * m + 2),
        out_specs=[pl.BlockSpec(memory_space=pltpu.VMEM)] * (len(direct) + m + 3),
        scratch_shapes=[
            *[pltpu.VMEM(half, f32) for half in halves * 2],
            *[pltpu.VMEM(half, bf16) for half in halves * 2],
            pltpu.VMEM((n, n * width), f32),
            pltpu.VMEM((width,), f32),
            pltpu.VMEM((width,), f32),
            pltpu.VMEM((1, n * width), f32),
            *[dma((count,))] * 2,
            dma((1 + m - smalls,)),
            dma((2,)),
            dma((6,)),
        ],
        compiler_params=pltpu.CompilerParams(
            collective_id=0, has_side_effects=True, vmem_limit_bytes=VMEM_BYTES - results - ROOM
        ),
        name="exchange",
    )(*slopes, slope_norm, *params, param_norm)
    swap = [(who, n - 1 - who) for who in range(n)]
    theirs = lax.ppermute(kept[0], "replica", swap)
    shapes = wholes + [(n * width,)] + halves + [(width,)]
    types = [bf16] * (m + 1) + [f32] * (m + 1)
    small_grant = pltpu.CompilerParams(vmem_limit_bytes=2 * 1024 * 1024)
    outs = list(pl.pallas_call(
        functools.partial(settle, by_row, halves, spots),
        out_shape=[jax.ShapeDtypeStruct(*out) for out in zip(shapes, types)],
        in_specs=[pl.BlockSpec(memory_space=pltpu.VMEM)] * len(kept),
        out_specs=[ANY] * len(shapes),
        scratch_shapes=[dma((len(kept),))],
        compiler_params=small_grant,
        cost_estimate=pl.CostEstimate(flops=10**8, bytes_accessed=results, transcendentals=0),
        name="settle",
    )(*kept))
    done = pl.pallas_call(
        functools.partial(finish, by_row, halves, spots),
        out_shape=[jax.ShapeDtypeStruct(outs[at].shape, outs[at].dtype) for at in spots],
        in_specs=[pl.BlockSpec(memory_space=pltpu.VMEM)] + [ANY] * len(spots),
        out_specs=[ANY] * len(spots),
        scratch_shapes=[dma(())],
        input_output_aliases={1 + k: k for k in range(len(spots))},
        compiler_params=small_grant,
        name="finish",
    )(theirs, *[outs[at] for at in spots])
    for at, whole in zip(spots, done):
        outs[at] = whole
    for at in turned:
        outs[at] = outs[at].T
        outs[m + 1 + at] = outs[m + 1 + at].T
    return tuple(outs)


def spread(
    slope_up,
    slope_down,
    slope_query,
    slope_key,
    slope_value,
    slope_mixed,
    slope_norm,
    param_up,
    param_down,
    param_query,
    param_key,
    param_value,
    param_mixed,
    param_norm,
):
    mean_up, mean_down, mean_query, mean_key, mean_value, mean_mixed = (
        lax.psum_scatter(slope_up[0], "replica", scatter_dimension=0, tiled=True),
        lax.psum_scatter(slope_down[0], "replica", scatter_dimension=1, tiled=True),
        lax.psum_scatter(slope_query[0], "replica", scatter_dimension=0, tiled=True),
        lax.psum_scatter(slope_key[0], "replica", scatter_dimension=0, tiled=True),
        lax.psum_scatter(slope_value[0], "replica", scatter_dimension=0, tiled=True),
        lax.psum_scatter(slope_mixed[0], "replica", scatter_dimension=1, tiled=True),
    )
    whole_norm = lax.psum(slope_norm[0], "replica")
    place = lax.axis_index("replica")
    mean_norm = lax.dynamic_slice_in_dim(
        whole_norm, place * param_norm.shape[0], param_norm.shape[0]
    )
    mean_rate = lax.axis_size("replica") ** (-0.5)
    mean_up = mean_up * mean_rate
    mean_down = mean_down * mean_rate
    mean_query = mean_query * mean_rate
    mean_key = mean_key * mean_rate
    mean_value = mean_value * mean_rate
    mean_mixed = mean_mixed * mean_rate
    mean_norm = mean_norm * mean_rate
    next_up = param_up - learn_rate * mean_up
    next_down = param_down - learn_rate * mean_down
    next_query = param_query - learn_rate * mean_query
    next_key = param_key - learn_rate * mean_key
    next_value = param_value - learn_rate * mean_value
    next_mixed = param_mixed - learn_rate * mean_mixed
    next_norm = param_norm - learn_rate * mean_norm
    half_up, half_down, half_query, half_key, half_value, half_mixed, half_norm = (
        lax.all_gather(next_up.astype(jnp.bfloat16), "replica", axis=0, tiled=True),
        lax.all_gather(next_down.astype(jnp.bfloat16), "replica", axis=1, tiled=True),
        lax.all_gather(next_query.astype(jnp.bfloat16), "replica", axis=0, tiled=True),
        lax.all_gather(next_key.astype(jnp.bfloat16), "replica", axis=0, tiled=True),
        lax.all_gather(next_value.astype(jnp.bfloat16), "replica", axis=0, tiled=True),
        lax.all_gather(next_mixed.astype(jnp.bfloat16), "replica", axis=1, tiled=True),
        lax.all_gather(next_norm.astype(jnp.bfloat16), "replica", axis=0, tiled=True),
    )
    return (
        half_up,
        half_down,
        half_query,
        half_key,
        half_value,
        half_mixed,
        half_norm,
        next_up,
        next_down,
        next_query,
        next_key,
        next_value,
        next_mixed,
        next_norm,
    )


def solution(mesh):
    placed = (
        P(("unit", "replica"), None, "model"),
        P(("unit", "replica"), "model", None),
        P(("unit", "replica"), None, "model"),
        P(("unit", "replica"), None, "model"),
        P(("unit", "replica"), None, "model"),
        P(("unit", "replica"), "model", None),
        P(("unit", "replica"), None),
        P(("unit", "replica"), "model"),
        P(("unit", "model"), "replica"),
        P(("unit", "replica"), "model"),
        P(("unit", "replica"), "model"),
        P(("unit", "replica"), "model"),
        P(("unit", "model"), "replica"),
        P(("unit", "replica")),
    )
    n = mesh.shape["replica"]
    return jax.shard_map(
        functools.partial(shards, n) if n == 2 else spread,
        mesh=mesh,
        in_specs=placed,
        out_specs=(
            P("unit", "model"),
            P(("unit", "model"), None),
            P("unit", "model"),
            P("unit", "model"),
            P("unit", "model"),
            P(("unit", "model"), None),
            P("unit"),
            P(("unit", "replica"), "model"),
            P(("unit", "model"), "replica"),
            P(("unit", "replica"), "model"),
            P(("unit", "replica"), "model"),
            P(("unit", "replica"), "model"),
            P(("unit", "model"), "replica"),
            P(("unit", "replica")),
        ),
        check_vma=False,
    )
```
